32 devices in a mesh: seq: 16 (over z, y, core), exp: 2 (over x).
Axes of the slice: x: 2, y: 2, z: 4, core: 2. Of those that a mesh axis runs over, the one named last changes fastest.
Arguments:
- hidden_in: bfloat16 [6, 6144], P('exp', 'seq'), may hold values from -2 to 2
- queries: bfloat16 [6, 6144], P(None, 'exp'), may hold values from -40 to 40
- key_cache: bfloat16 [6, 8192, 1024], P(None, 'seq', 'exp'), may hold values from -16 to 16
- value_cache: bfloat16 [6, 8192, 1024], P(None, 'seq', 'exp'), may hold values from -6 to 6
- lengths: int32 [6], replicated, may hold values from 2 to 8192
- out_weight: bfloat16 [6144, 6144], P('exp', 'seq'), may hold values from -0.078125 to 0.078125
- norm_gain: float32 [6144], P('seq'), may hold values from 0.1 to 1.9
- router: bfloat16 [6144, 8], P('seq'), may hold values from -0.078125 to 0.078125
- expert_ids: int32 [6, 2], P('exp'), may hold values from 0 to 7, as said below
- capacity: int32 [8], replicated, may hold values from 1 to 3, as said below
- w_gate: bfloat16 [8, 6144, 8192], P('exp', None, 'seq'), may hold values from -0.078125 to 0.078125
- w_up: bfloat16 [8, 6144, 8192], P('exp', None, 'seq'), may hold values from -0.078125 to 0.078125
- w_down: bfloat16 [8, 8192, 6144], P('exp', 'seq'), may hold values from -0.09375 to 0.09375
Outputs:
- layer_out: bfloat16 [6, 6144], P('exp', 'seq')
The draws below stay inside these ranges and needn't reach their ends.
Inputs may be any that keep to these rules, and one draw needn't show every extreme that they name: lengths[b] counts sequence b's live cache positions, the newest token's included. `expert_ids`: the two experts of a token differ. One expert is named by every token; any other expert is named at most 3 times within one aligned block of 3 tokens. The expert that every token names has capacity 3.
All inputs are finite; a program needn't handle non-finite values.
Results may differ from the reference program's by a relative error of at most 0.0085.
Values may be sent and summed in bfloat16 or wider, within the bound.
A program may use at most 128 MiB of HBM per device.

```python
import math
import jax
import jax.numpy as jnp
from jax import lax

D = 6144
HEADS = 48
KV_HEADS = 8
HEAD_DIM = 128
EXPERTS = 8
FF_W = 8192
TOK_DEV = 3
LENGTH = 8192
SEQS = 6


def hot_expert(key):
    return jax.random.randint(jax.random.fold_in(key, 11), (), 0, EXPERTS)


def draw_expert_ids(key, part):
    favored = hot_expert(key)
    offsets = jax.random.randint(jax.random.fold_in(key, 12), (SEQS,), 1, EXPERTS)
    other_ids = (favored + offsets) % EXPERTS
    flipped = jax.random.randint(jax.random.fold_in(key, 13), (SEQS,), 0, 2)
    first_ids = jnp.where(flipped == 1, other_ids, favored)
    second_ids = jnp.where(flipped == 1, favored, other_ids)
    return jnp.stack([first_ids, second_ids], axis=1).astype(jnp.int32)


def draw_capacity(key, part):
    favored = hot_expert(key)
    limits = jax.random.randint(jax.random.fold_in(key, 14), (EXPERTS,), 1, TOK_DEV + 1)
    return jnp.where(jnp.arange(EXPERTS) == favored, TOK_DEV, limits).astype(jnp.int32)


def draw_queries(key, part):
    return jnp.clip(2.5 * jax.random.normal(jax.random.fold_in(key, 32), (SEQS, HEADS * HEAD_DIM), jnp.float32), -15.0, 15.0).astype(jnp.bfloat16)


def draw_key_cache(key, part):
    key_rows = jnp.clip(jax.random.normal(jax.random.fold_in(key, 33), (SEQS, LENGTH, KV_HEADS * HEAD_DIM), jnp.float32), -6.0, 6.0)
    return key_rows.astype(jnp.bfloat16)


def touch_ends(values, rng, least, largest):
    extent = values.shape
    place = [jax.random.randint(jax.random.fold_in(rng, axis), (), 0, extent[axis]) for axis in range(len(extent))]
    values = values.at[tuple(place)].set(least)
    longest = extent.index(max(extent))
    place[longest] = (place[longest] + 1) % extent[longest]
    return values.at[tuple(place)].set(largest)


def spiked(result, stream_key, source, target, parts, factor):
    def block_of(axis_at):
        return (jnp.arange(result.shape[axis_at]) // (result.shape[axis_at] // parts)).reshape((-1,) + (1,) * (result.ndim - 1 - axis_at))

    near = jax.random.permutation(stream_key, parts)[block_of(target)]
    second = (block_of(target) + parts // 2) % parts
    return jnp.where((block_of(source) == near) | (block_of(source) == second), factor * result, result)


def level_of(own_key, shape, split, smallest, largest):
    level = 1.0
    for axis_at, shards_of in split:
        draws = jax.random.uniform(jax.random.fold_in(jax.random.fold_in(own_key, 6), axis_at), (shards_of,), jnp.float32, smallest / len(split), largest / len(split))
        level = level * jnp.repeat(jnp.exp(draws), shape[axis_at] // shards_of).reshape((-1,) + (1,) * (len(shape) - 1 - axis_at))
    return level


def centred(own_key, dims, scale, most, shards=(), held_as=jnp.bfloat16):
    drawn = scale * jax.random.normal(own_key, dims, jnp.float32)
    if shards:
        drawn = drawn * level_of(own_key, dims, shards, -0.22, 0.18)
    return jnp.clip(drawn, -most, most).astype(held_as)


def heavy_noise(own_key, extent, width, limit, shards, heavy, kind=jnp.bfloat16):
    array = width * jax.random.normal(own_key, extent, jnp.float32)
    if shards:
        array = array * level_of(own_key, extent, shards, -0.22, 0.18)
    return jnp.clip(spiked(array, jax.random.fold_in(own_key, 3), *heavy), -limit, limit).astype(kind)


def setup_inputs(seed: int = 0) -> dict:
    arg_keys = jax.random.split(jax.random.key(seed), 14)
    return {
        "hidden_in": centred(arg_keys[0], (SEQS, D), 0.3, 2.0, ((0, 2), (1, 16))),
        "queries": draw_queries(jax.random.fold_in(arg_keys[13], 71), 0),
        "key_cache": draw_key_cache(jax.random.fold_in(arg_keys[13], 71), 0),
        "value_cache": centred(arg_keys[3], (SEQS, LENGTH, KV_HEADS * HEAD_DIM), 1.0, 6.0, ((1, 16), (2, 2))),
        "lengths": touch_ends(jax.random.randint(arg_keys[4], (SEQS,), 2, LENGTH + 1), jax.random.fold_in(arg_keys[4], 1), 2, LENGTH).astype(jnp.int32),
        "out_weight": centred(arg_keys[5], (HEADS * HEAD_DIM, D), (HEADS * HEAD_DIM) ** -0.5, 0.078125, ((0, 2), (1, 16))),
        "norm_gain": jnp.clip(1.0 + 0.18 * jax.random.normal(arg_keys[6], (D,), jnp.float32), 0.1, 1.9),
        "router": centred(arg_keys[7], (D, EXPERTS), D ** -0.5, 0.078125, ((0, 16),)),
        "expert_ids": draw_expert_ids(jax.random.fold_in(arg_keys[13], 71), 0),
        "capacity": draw_capacity(jax.random.fold_in(arg_keys[13], 71), 0),
        "w_gate": centred(arg_keys[10], (EXPERTS, D, FF_W), D ** -0.5, 0.078125, ((0, 2), (2, 16))),
        "w_up": centred(arg_keys[11], (EXPERTS, D, FF_W), D ** -0.5, 0.078125, ((0, 2), (2, 16))),
        "w_down": heavy_noise(arg_keys[12], (EXPERTS, FF_W, D), FF_W ** -0.5, 0.09375, ((0, 2), (1, 16)), (1, 2, 16, 2.0)),
    }


masked_score = -1e+30
norm_eps = 1e-05

def expert_rows(normed, gate_mat, up_mat, down_weight_matrix):
    gate_sum = jnp.dot(normed, gate_mat, preferred_element_type=jnp.float32)
    up_sum = jnp.dot(normed, up_mat, preferred_element_type=jnp.float32)
    hidden_act = (jax.nn.silu(gate_sum) * up_sum).astype(jnp.bfloat16)
    return jnp.dot(hidden_act, down_weight_matrix, preferred_element_type=jnp.float32)

def reference(hidden_in, queries, key_cache, value_cache, lengths, out_weight, norm_gain, router, expert_ids, capacity, w_gate, w_up, w_down):
    group_size = HEADS // KV_HEADS
    query_heads = queries.astype(jnp.float32).reshape(SEQS, KV_HEADS, group_size, HEAD_DIM)
    positions = jnp.arange(LENGTH, dtype=jnp.int32)
    live_mask = positions[None, :] < lengths[:, None]
    outputs = []
    for kv_index in range(KV_HEADS):
        key_rows = key_cache[:, :, kv_index * HEAD_DIM:(kv_index + 1) * HEAD_DIM].astype(jnp.float32)
        value_rows = value_cache[:, :, kv_index * HEAD_DIM:(kv_index + 1) * HEAD_DIM].astype(jnp.float32)
        scores = jnp.einsum('bgd,bjd->bgj', query_heads[:, kv_index], key_rows, precision=lax.Precision.HIGHEST) * (1.0 / math.sqrt(HEAD_DIM))
        scores = jnp.where(live_mask[:, None, :], scores, masked_score)
        peak_score = lax.optimization_barrier(jnp.max(scores, axis=-1, keepdims=True))
        attn_weights = jnp.where(live_mask[:, None, :], jnp.exp(scores - peak_score), 0.0)
        denom_sum = lax.optimization_barrier(jnp.sum(attn_weights, axis=-1))
        weighted = jnp.einsum('bgj,bjd->bgd', attn_weights, value_rows, precision=lax.Precision.HIGHEST)
        outputs.append(weighted / denom_sum[..., None])
    attended = jnp.stack(outputs, axis=1).reshape(SEQS, HEADS * HEAD_DIM).astype(jnp.bfloat16)
    projected = jnp.dot(attended, out_weight, preferred_element_type=jnp.float32)
    residual = hidden_in.astype(jnp.float32) + projected
    scale_row = lax.rsqrt(lax.optimization_barrier(jnp.sum(residual * residual, axis=-1)) / D + norm_eps)
    gained = residual * norm_gain
    logits = jnp.dot(gained, router.astype(jnp.float32), precision=lax.Precision.HIGHEST) * scale_row[:, None]
    normed = (gained * scale_row[:, None]).astype(jnp.bfloat16)
    onehot_int = (expert_ids[:, :, None] == jnp.arange(EXPERTS, dtype=jnp.int32)[None, None, :]).astype(jnp.int32)
    name_count = lax.optimization_barrier(jnp.sum(onehot_int, axis=1))
    row_order = jnp.arange(SEQS, dtype=jnp.int32)
    row_block = row_order // TOK_DEV
    before = ((row_block[:, None] == row_block[None, :]) & (row_order[None, :] < row_order[:, None])).astype(jnp.int32)
    earlier = jnp.dot(before, name_count)
    slot_rank = lax.optimization_barrier(jnp.sum(onehot_int * earlier[:, None, :], axis=-1))
    slot_limit = lax.optimization_barrier(jnp.sum(onehot_int * capacity[None, None, :], axis=-1))
    kept_mask = (slot_rank < slot_limit).astype(jnp.float32)
    expert_indicator = onehot_int.astype(jnp.float32)
    chosen = lax.optimization_barrier(jnp.sum(expert_indicator * logits[:, None, :], axis=-1))
    gate_weight = jax.nn.sigmoid(chosen - chosen[:, ::-1])
    expert_output = lax.map(lambda mats: expert_rows(normed, mats[0], mats[1], mats[2]), (w_gate, w_up, w_down))
    selected_experts = jnp.einsum('hlw,whv->hlv', expert_indicator, expert_output, precision=lax.Precision.HIGHEST)
    combined = lax.optimization_barrier(jnp.sum((gate_weight * kept_mask)[:, :, None] * selected_experts, axis=1))
    return (residual + combined).astype(jnp.bfloat16)
```

```python
import functools
import math

import jax
import jax.numpy as jnp
from jax import lax
from jax.experimental import pallas as pl
from jax.experimental.pallas import tpu as pltpu
from jax.sharding import PartitionSpec as P

MESH = pl.DeviceIdType.MESH
HEAD_DIM = 128
LANES = 128
masked_score = -1e30
norm_eps = 1e-05
F32 = jnp.float32
BF16 = jnp.bfloat16


def up(value, step):
    return -(-value // step) * step


def iota(shape, axis):
    return lax.broadcasted_iota(jnp.int32, shape, axis)


def div(value, by):
    return lax.div(value, jnp.full_like(value, by))


def rem(value, by):
    return lax.rem(value, jnp.full_like(value, by))


def dot(a, b):
    return jnp.dot(a, b, preferred_element_type=F32)


def attend_kernel(len_ref, q_ref, k_ref, v_ref, o_ref):
    b = pl.program_id(0)
    span = k_ref.shape[1]
    kvl, gp = q_ref.shape[1], q_ref.shape[2]
    first = lax.axis_index("seq") * span
    live = (iota((gp, span), 1) + first) < len_ref[b]
    lane = iota((gp, LANES), 1)
    for kv in range(kvl):
        cols = slice(kv * HEAD_DIM, (kv + 1) * HEAD_DIM)
        s = lax.dot_general(
            q_ref[0, kv], k_ref[0, :, cols], (((1,), (1,)), ((), ())), preferred_element_type=F32
        ) * (1.0 / math.sqrt(HEAD_DIM))
        s = jnp.where(live, s, masked_score)
        m = jnp.max(s, axis=1, keepdims=True).astype(BF16).astype(F32)
        w = jnp.where(live, jnp.exp(s - m), 0.0)
        l = jnp.sum(w, axis=1, keepdims=True)
        acc = dot(w.astype(BF16), v_ref[0, :, cols])
        l_hi = l.astype(BF16).astype(F32)
        stats = jnp.where(lane == 0, m, jnp.where(lane == 1, l_hi, jnp.where(lane == 2, l - l_hi, 0.0)))
        rows = slice(kv * gp, (kv + 1) * gp)
        o_ref[rows, :HEAD_DIM] = acc.astype(BF16)
        o_ref[rows, HEAD_DIM:] = stats.astype(BF16)


def ring_of(axis, count):
    me = lax.axis_index(axis)
    return me, [lax.rem(me + k, count) for k in range(count)], [lax.rem(me + count - k, count) for k in range(count)]


def merge_kernel(
    dims, x_ref, ids_ref, ow_hbm, hid_ref, gain_ref, rt_ref,
    xg_ref, st_ref, idv_ref, res_ref,
    ow, send1, recv1, buf2, buf3, buf4,
    ow_sem, ss1, rs1, ss2, rs2, ss3, rs3, ss4, rs4,
):
    n_seq, n_exp, seqs, toks, kvl, group, rv, rp = dims
    gp = up(group, 8)
    heads = kvl * group
    bp = buf3.shape[1]
    width = hid_ref.shape[1]
    me, to_seq, from_seq = ring_of("seq", n_seq)
    my_e, to_exp, from_exp = ring_of("exp", n_exp)

    barrier = pltpu.get_barrier_semaphore()
    for k in range(1, n_seq):
        pl.semaphore_signal(barrier, inc=1, device_id={"seq": to_seq[k]}, device_id_type=MESH)
    for k in range(1, n_exp):
        pl.semaphore_signal(barrier, inc=1, device_id={"exp": to_exp[k]}, device_id_type=MESH)
    ow_copy = pltpu.make_async_copy(ow_hbm, ow, ow_sem)
    ow_copy.start()

    src = iota((1, x_ref.shape[0]), 1)
    src_h = rem(src, kvl * gp)
    src_g = rem(src_h, gp)
    src_row = div(src, kvl * gp) * heads + div(src_h, gp) * group + src_g
    src_row = jnp.where(src_g < group, src_row, -1)
    slot = iota((n_seq * rp, 1), 0)
    slot_k = rem(slot, rp)
    slot_row = jnp.where(slot_k < rv, div(slot, rp) * rv + slot_k, -2)
    pack = (slot_row == src_row).astype(F32).astype(BF16)
    packed = dot(pack, x_ref[...]).astype(BF16)
    for p in range(n_seq):
        send1[p] = packed[p * rp:(p + 1) * rp]
    recv1[me] = send1[me]
    pl.semaphore_wait(barrier, n_seq + n_exp - 2)

    out1 = []
    for k in range(1, n_seq):
        c = pltpu.make_async_remote_copy(
            send1.at[to_seq[k]], recv1.at[me], ss1.at[k], rs1.at[k],
            device_id={"seq": to_seq[k]}, device_id_type=MESH)
        c.start()
        out1.append(c)
    for k in range(1, n_seq):
        pltpu.make_async_remote_copy(
            send1.at[to_seq[k]], recv1.at[from_seq[k]], ss1.at[k], rs1.at[k],
            device_id={"seq": to_seq[k]}, device_id_type=MESH).wait_recv()
    stats = [recv1[p][:, HEAD_DIM:].astype(F32) for p in range(n_seq)]
    peaks = [s[:, 0:1] for s in stats]
    top = functools.reduce(jnp.maximum, peaks)
    acc = jnp.zeros((rp, HEAD_DIM), F32)
    den = jnp.zeros((rp, 1), F32)
    for p in range(n_seq):
        f = jnp.exp(peaks[p] - top)
        den = den + (stats[p][:, 1:2] + stats[p][:, 2:3]) * f
        acc = acc + recv1[p][:, :HEAD_DIM].astype(F32) * f
    att = jnp.where(den > 0.0, acc / jnp.where(den > 0.0, den, 1.0), 0.0)
    buf2[me] = att.astype(BF16)

    def gather(buf, sends, recvs, axis, mine, to, frm):
        started = []
        for k in range(1, len(to)):
            c = pltpu.make_async_remote_copy(
                buf.at[mine], buf.at[mine], sends.at[k], recvs.at[k],
                device_id={axis: to[k]}, device_id_type=MESH)
            c.start()
            started.append(c)
        for k in range(1, len(to)):
            pltpu.make_async_remote_copy(
                buf.at[mine], buf.at[frm[k]], sends.at[k], recvs.at[k],
                device_id={axis: to[k]}, device_id_type=MESH).wait_recv()
        return started

    out2 = gather(buf2, ss2, rs2, "seq", me, to_seq, from_seq)
    row = iota((heads * bp, 1), 0)
    row_b = rem(row, bp)
    want = jnp.where(row_b < seqs, row_b * heads + div(row, bp), -3)
    slot = iota((1, n_seq * rp), 1)
    slot_k = rem(slot, rp)
    have = jnp.where(slot_k < rv, div(slot, rp) * rv + slot_k, -2)
    unpack = (want == have).astype(F32).astype(BF16)
    rows = dot(unpack, jnp.concatenate([buf2[p] for p in range(n_seq)], axis=0))
    att_all = jnp.concatenate([rows[h * bp:(h + 1) * bp] for h in range(heads)], axis=1).astype(BF16)
    ow_copy.wait()
    part = dot(att_all, ow[...])
    hid = hid_ref[...].astype(F32)
    rowc = iota((bp, width), 0)
    rowl = iota((bp, LANES), 0)
    lane = iota((bp, LANES), 1)
    idv = jnp.zeros((bp, LANES), F32)
    for t in range(toks):
        at = my_e * toks + t
        part = part + jnp.where(rowc == at, hid[t:t + 1, :], 0.0)
        for k in range(2):
            idv = idv + jnp.where((rowl == at) & (lane == k), ids_ref[t, k].astype(F32), 0.0)
    buf3[my_e, :, :width] = part
    buf3[my_e, :, width:] = idv
    out3 = gather(buf3, ss3, rs3, "exp", my_e, to_exp, from_exp)
    total = functools.reduce(lambda a, b: a + b, [buf3[e] for e in range(n_exp)])
    residual = total[:, :width]
    idv_ref[...] = total[:, width:].astype(jnp.int32)
    for t in range(toks):
        mine = jnp.sum(jnp.where(rowc == my_e * toks + t, residual, 0.0), axis=0, keepdims=True)
        res_ref[t:t + 1, :] = mine
    gained = residual * gain_ref[...]
    logit = jnp.dot(gained, rt_ref[...].astype(F32), precision=lax.Precision.HIGHEST, preferred_element_type=F32)
    square = jnp.sum(residual * residual, axis=1, keepdims=True)
    st = jnp.where(lane == 15, square, logit)
    hi = st.astype(BF16).astype(F32)
    buf4[me, :, :width] = gained.astype(BF16)
    buf4[me, :, width:] = (hi + pltpu.roll(st - hi, 16, 1)).astype(BF16)
    out4 = gather(buf4, ss4, rs4, "seq", me, to_seq, from_seq)
    tot = jnp.zeros((bp, LANES), F32)
    for p in range(n_seq):
        xg_ref[:, p * width:(p + 1) * width] = buf4[p, :, :width]
        tot = tot + buf4[p, :, width:].astype(F32)
    st_ref[...] = tot + pltpu.roll(tot, LANES - 16, 1)
    for c in out1 + out2 + out3 + out4:
        c.wait_send()


def expert_kernel(
    dims, ids_ref, cap_ref, xg_ref, st_ref, idv_ref, wg_hbm, wu_hbm, wd_hbm,
    o_ref, gate, upb, down, y, coef, order, sems,
):
    n_seq, n_exp, seqs, toks, n_experts, chunk = dims
    local = wg_hbm.shape[0]
    bp, model = xg_ref.shape
    width = model // n_seq
    slots = gate.shape[0]
    chunks = wg_hbm.shape[2] // chunk
    first = lax.axis_index("exp") * local

    count = jnp.int32(0)
    for e in range(local):
        named = jnp.int32(0)
        for b in range(seqs):
            for k in range(2):
                named = named | (ids_ref[b, k] == first + e).astype(jnp.int32)

        @pl.when(named > 0)
        def _():
            order[count] = e

        count = count + named
    steps = count * chunks

    def copies(i):
        s = lax.rem(i, slots)
        e = order[lax.div(i, chunks)]
        at = pl.multiple_of(lax.rem(i, chunks) * chunk, chunk)
        return (
            pltpu.make_async_copy(wg_hbm.at[e, :, pl.ds(at, chunk)], gate.at[s], sems.at[s, 0]),
            pltpu.make_async_copy(wu_hbm.at[e, :, pl.ds(at, chunk)], upb.at[s], sems.at[s, 1]),
            pltpu.make_async_copy(wd_hbm.at[e, pl.ds(at, chunk), :], down.at[s], sems.at[s, 2]),
        )

    for i in range(slots - 1):
        @pl.when(i < steps)
        def _():
            for c in copies(jnp.int32(i)):
                c.start()

    st = st_ref[...]
    lane = iota((bp, LANES), 1)
    rowc = iota((bp, 1), 0)
    scale = lax.rsqrt(st[:, 15:16] / model + norm_eps)
    logits = jnp.where(lane < n_experts, st, 0.0) * scale
    ids = [idv_ref[:, k:k + 1] for k in range(2)]
    chosen = [jnp.sum(jnp.where(lane == ids[k], logits, 0.0), axis=1, keepdims=True) for k in range(2)]
    weight = []
    for k in range(2):
        rank = jnp.zeros((bp, 1), jnp.int32)
        for b in range(seqs):
            end = (b // toks + 1) * toks
            later = (rowc > b) & (rowc < end)
            for j in range(2):
                rank = rank + jnp.where(later & (ids[k] == ids_ref[b, j]), 1, 0)
        limit = jnp.zeros((bp, 1), jnp.int32)
        for e in range(n_experts):
            limit = limit + jnp.where(ids[k] == e, cap_ref[e], 0)
        keep = (rank < limit) & (rowc < seqs)
        weight.append(jnp.where(keep, jax.nn.sigmoid(chosen[k] - chosen[1 - k]), 0.0))
    coef[0] = jnp.broadcast_to(weight[0], (bp, LANES))
    coef[1] = jnp.broadcast_to(weight[1], (bp, LANES))
    y[...] = jnp.zeros_like(y)

    def step(i, carry):
        for c in copies(i):
            c.wait()

        @pl.when(i + slots - 1 < steps)
        def _():
            for c in copies(i + slots - 1):
                c.start()

        s = lax.rem(i, slots)
        e = order[lax.div(i, chunks)] + first
        x = xg_ref[...]
        g = dot(x, gate[s]) * scale
        u = dot(x, upb[s]) * scale
        h = (jax.nn.silu(g) * u).astype(BF16)
        c = jnp.where(ids[0] == e, coef[0][:, :1], 0.0) + jnp.where(ids[1] == e, coef[1][:, :1], 0.0)
        y[...] += dot(h, down[s]) * c
        return carry

    lax.fori_loop(0, steps, step, jnp.int32(0))
    for e in range(n_exp):
        rows = y[e * toks:(e + 1) * toks, :].astype(BF16)
        for s in range(n_seq):
            o_ref[e * n_seq + s] = rows[:, s * width:(s + 1) * width]


def scatter_kernel(dims, y_ref, res_ref, o_ref, recv, ss, rs):
    n_seq, n_exp = dims
    n = n_seq * n_exp
    me = lax.axis_index("exp") * n_seq + lax.axis_index("seq")
    to = [lax.rem(me + k, n) for k in range(n)]
    frm = [lax.rem(me + n - k, n) for k in range(n)]

    def where(p):
        return {"seq": lax.rem(p, n_seq), "exp": lax.div(p, n_seq)}

    barrier = pltpu.get_barrier_semaphore()
    for k in range(1, n):
        pl.semaphore_signal(barrier, inc=1, device_id=where(to[k]), device_id_type=MESH)
    recv[me] = y_ref[me]
    pl.semaphore_wait(barrier, n - 1)
    started = []
    for k in range(1, n):
        c = pltpu.make_async_remote_copy(
            y_ref.at[to[k]], recv.at[me], ss.at[k], rs.at[k],
            device_id=where(to[k]), device_id_type=MESH)
        c.start()
        started.append(c)
    for k in range(1, n):
        pltpu.make_async_remote_copy(
            y_ref.at[to[k]], recv.at[frm[k]], ss.at[k], rs.at[k],
            device_id=where(to[k]), device_id_type=MESH).wait_recv()
    total = res_ref[...]
    for p in range(n):
        total = total + recv[p].astype(F32)
    o_ref[...] = total.astype(BF16)
    for c in started:
        c.wait_send()


def on_device(
    n_seq, n_exp, hidden_in, queries, key_cache, value_cache, lengths, out_weight, norm_gain,
    router, expert_ids, capacity, w_gate, w_up, w_down,
):
    seqs = queries.shape[0]
    toks, width = hidden_in.shape
    span = key_cache.shape[1]
    kvl = key_cache.shape[2] // HEAD_DIM
    heads = queries.shape[1] // HEAD_DIM
    group = heads // kvl
    gp = up(group, 8)
    bp = up(seqs, 8)
    n_experts = router.shape[1]
    model = width * n_seq
    rv = -(-seqs * heads // n_seq)
    rp = up(rv, 16)
    vmem = pl.BlockSpec(memory_space=pltpu.VMEM)
    smem = pl.BlockSpec(memory_space=pltpu.SMEM)
    hbm = pl.BlockSpec(memory_space=pltpu.HBM)
    q = jnp.pad(queries.reshape(seqs, kvl, group, HEAD_DIM), ((0, 0), (0, 0), (0, gp - group), (0, 0)))
    partial = pl.pallas_call(
        attend_kernel,
        grid=(seqs,),
        in_specs=[
            smem,
            pl.BlockSpec((1, kvl, gp, HEAD_DIM), lambda b: (b, 0, 0, 0)),
            pl.BlockSpec((1, span, kvl * HEAD_DIM), lambda b: (b, 0, 0)),
            pl.BlockSpec((1, span, kvl * HEAD_DIM), lambda b: (b, 0, 0)),
        ],
        out_specs=pl.BlockSpec((kvl * gp, 2 * HEAD_DIM), lambda b: (b, 0)),
        out_shape=jax.ShapeDtypeStruct((seqs * kvl * gp, 2 * HEAD_DIM), BF16),
        name="attend",
    )(lengths, q, key_cache, value_cache)

    dma = pltpu.SemaphoreType.DMA
    rt = jnp.pad(router, ((0, 0), (0, LANES - n_experts)))
    xg, st, idv, res = pl.pallas_call(
        functools.partial(merge_kernel, (n_seq, n_exp, seqs, toks, kvl, group, rv, rp)),
        in_specs=[vmem, smem, hbm, vmem, vmem, vmem],
        out_specs=[vmem] * 4,
        out_shape=[
            jax.ShapeDtypeStruct((bp, model), BF16),
            jax.ShapeDtypeStruct((bp, LANES), F32),
            jax.ShapeDtypeStruct((bp, LANES), jnp.int32),
            jax.ShapeDtypeStruct((toks, width), F32),
        ],
        scratch_shapes=[
            pltpu.VMEM(out_weight.shape, BF16),
            pltpu.VMEM((n_seq, rp, 2 * HEAD_DIM), BF16),
            pltpu.VMEM((n_seq, rp, 2 * HEAD_DIM), BF16),
            pltpu.VMEM((n_seq, rp, HEAD_DIM), BF16),
            pltpu.VMEM((n_exp, bp, width + LANES), F32),
            pltpu.VMEM((n_seq, bp, width + LANES), BF16),
            dma,
            dma((n_seq,)), dma((n_seq,)), dma((n_seq,)), dma((n_seq,)),
            dma((n_exp,)), dma((n_exp,)), dma((n_seq,)), dma((n_seq,)),
        ],
        compiler_params=pltpu.CompilerParams(collective_id=0, has_side_effects=True),
        name="merge",
    )(partial, expert_ids, out_weight, hidden_in, norm_gain.reshape(1, width), rt)

    chunk = min(256, w_gate.shape[2])
    slots = 3
    y = pl.pallas_call(
        functools.partial(expert_kernel, (n_seq, n_exp, seqs, toks, n_experts, chunk)),
        in_specs=[smem, smem, vmem, vmem, vmem, hbm, hbm, hbm],
        out_specs=vmem,
        out_shape=jax.ShapeDtypeStruct((n_exp * n_seq, toks, width), BF16),
        scratch_shapes=[
            pltpu.VMEM((slots, model, chunk), BF16),
            pltpu.VMEM((slots, model, chunk), BF16),
            pltpu.VMEM((slots, chunk, model), BF16),
            pltpu.VMEM((bp, model), F32),
            pltpu.VMEM((2, bp, LANES), F32),
            pltpu.SMEM((w_gate.shape[0],), jnp.int32),
            dma((slots, 3)),
        ],
        compiler_params=pltpu.CompilerParams(vmem_limit_bytes=48 * 1024 * 1024),
        name="experts",
    )(idv, capacity, xg, st, idv, w_gate, w_up, w_down)

    return pl.pallas_call(
        functools.partial(scatter_kernel, (n_seq, n_exp)),
        in_specs=[vmem, vmem],
        out_specs=vmem,
        out_shape=jax.ShapeDtypeStruct((toks, width), BF16),
        scratch_shapes=[
            pltpu.VMEM((n_exp * n_seq, toks, width), BF16),
            dma((n_exp * n_seq,)), dma((n_exp * n_seq,)),
        ],
        compiler_params=pltpu.CompilerParams(collective_id=1, has_side_effects=True),
        name="scatter",
    )(y, res)


def solution(mesh):
    in_specs = (
        P("exp", "seq"),
        P(None, "exp"),
        P(None, "seq", "exp"),
        P(None, "seq", "exp"),
        P(),
        P("exp", "seq"),
        P("seq"),
        P("seq", None),
        P("exp", None),
        P(),
        P("exp", None, "seq"),
        P("exp", None, "seq"),
        P("exp", "seq", None),
    )
    return jax.shard_map(
        functools.partial(on_device, mesh.shape["seq"], mesh.shape["exp"]),
        mesh=mesh, in_specs=in_specs, out_specs=P("exp", "seq"), check_vma=False,
    )
```
